16 devices in a mesh: dp: 4 (over y, z, core), sp: 4 (over x).
Axes of the slice: x: 4, y: 2, z: 1, core: 2. Of those that a mesh axis runs over, the one named last changes fastest.
The devices are a block of a 4x4x8 slice.
Arguments:
- x: bfloat16 [16384, 5120], P(('dp', 'sp')), parts along dimension 0
- gain: bfloat16 [5120], replicated
- wq: bfloat16 [5120, 4096], P('sp')
- wk: bfloat16 [5120, 1024], P('sp')
- wv: bfloat16 [5120, 1024], P('sp')
- wo: bfloat16 [4096, 5120], P('sp')
Outputs:
- output: bfloat16 [16384, 5120], P(('dp', 'sp')), parts along dimension 0
There are 4 independent parts. The reference program is written for one: setup_inputs(seed, part) draws one part's arguments, and reference() takes and returns one part's arrays. A program takes and returns all parts, laid end to end along the dimension named above; an argument that names none is the same for every part.
All inputs are finite; a program needn't handle non-finite values.
Results may differ from the reference program's by a relative error of at most 0.012.
Values are sent between devices in bfloat16 or wider.
A program may use at most 768 MiB of HBM per device.

```python
import jax
import jax.numpy as jnp
from jax import lax

ROWS = 4096
D = 5120
HEADS = 32
KV_HEADS = 8
HEAD = 128
THETA = 10000


def setup_inputs(seed: int = 0, part: int = 0) -> dict:
    kx, kn, kq, kk, kv, ko = jax.random.split(jax.random.key(seed), 6)

    def weights(key, rows, columns):
        return jax.random.normal(key, (rows, columns), jnp.float32) * rows**-0.5

    drawn = {
        "x": jax.random.normal(jax.random.fold_in(kx, part), (ROWS, D), jnp.float32),
        "gain": 1 + 0.1 * jax.random.normal(kn, (D,), jnp.float32),
        "wq": 2 * weights(kq, D, HEADS * HEAD),
        "wk": 2 * weights(kk, D, KV_HEADS * HEAD),
        "wv": 4 * weights(kv, D, KV_HEADS * HEAD),
        "wo": weights(ko, HEADS * HEAD, D),
    }
    return {k: v.astype(jnp.bfloat16) for k, v in drawn.items()}


def normed(x, gain):
    wide = x.astype(jnp.float32)
    scale = lax.rsqrt(jnp.mean(wide * wide, -1, keepdims=True) + 1e-6)
    return (wide * scale * gain.astype(jnp.float32)).astype(jnp.bfloat16)


def turned(t, place, theta):
    half = t.shape[-1] // 2
    angle = place.astype(jnp.float32)[:, None] * theta ** (-jnp.arange(half, dtype=jnp.float32) / half)
    cos, sin = jnp.cos(angle)[:, None], jnp.sin(angle)[:, None]
    a, b = t[..., :half].astype(jnp.float32), t[..., half:].astype(jnp.float32)
    return jnp.concatenate([a * cos - b * sin, b * cos + a * sin], -1).astype(jnp.bfloat16)


def matmul(a, w):
    return jnp.dot(a, w, preferred_element_type=jnp.float32).astype(jnp.bfloat16)


def einsum(form, a, b):
    return jnp.einsum(form, a.astype(jnp.float32), b.astype(jnp.float32))


def attention(q, k, v):
    scores = einsum("tgsd,ugd->gstu", q, k) * q.shape[-1] ** -0.5
    token = jnp.arange(q.shape[0])
    scores = jnp.where(token[:, None] >= token, scores, -jnp.inf)
    weights = jax.nn.softmax(scores, -1).astype(jnp.bfloat16)
    return einsum("gstu,ugd->tgsd", weights, v).astype(jnp.bfloat16)


def reference(x, gain, wq, wk, wv, wo):
    a, place = normed(x, gain), jnp.arange(ROWS)
    q = turned(matmul(a, wq).reshape(ROWS, HEADS, HEAD), place, THETA).reshape(ROWS, KV_HEADS, -1, HEAD)
    k = turned(matmul(a, wk).reshape(ROWS, KV_HEADS, HEAD), place, THETA)
    v = matmul(a, wv).reshape(ROWS, KV_HEADS, HEAD)
    seen = attention(q, k, v).reshape(ROWS, HEADS * HEAD)
    return (x.astype(jnp.float32) + jnp.dot(seen, wo, preferred_element_type=jnp.float32)).astype(jnp.bfloat16)
```

```python
import functools

import jax
import jax.numpy as jnp
from jax import lax
from jax.experimental import pallas as pl
from jax.experimental.pallas import tpu as pltpu
from jax.sharding import PartitionSpec as P

NEG = -1e30
HIDDEN = 2 * NEG
LOG2E = 1.4426950408889634
VMEM = 67043328
HEAD = 128
THETA = 10000
STRIP = 512
WO_COLS = 512
TILE = 256
NORM_ROWS = 128
MESH = pl.DeviceIdType.MESH
F32, BF16 = jnp.float32, jnp.bfloat16


def _dot(a, b, ca, cb):
    return lax.dot_general(a, b, (((ca,), (cb,)), ((), ())), preferred_element_type=F32)


def _shared(rows, alone):
    return rows - alone, alone


def kernel(dims, x_ref, gain_ref, cos_ref, sin_ref, wq_ref, wk_ref, wv_ref, wo_ref,
           y_ref, gw_ref, go_ref, kall_ref, vall_ref,
           a_s, w_s, t_s, q_s, kst, vst, k_s, v_s, seen_s, top_s, mix_s, xb, xr, yb,
           send, recv, ksend, krecv, wl, kl, xl, rl, yl):
    n, groups, share, nq, no, alone_q, alone_o = dims
    own, width = x_ref.shape
    rows_q, rows_o = wq_ref.shape[0], wo_ref.shape[0]
    qcols = share * HEAD
    ccols = qcols + 2 * HEAD
    me, dp = lax.axis_index("sp"), lax.axis_index("dp")
    right, left = lax.rem(me + 1, n), lax.rem(me + n - 1, n)
    across = lax.rem(me + 2, n)
    core, pair = lax.rem(dp, 2), lax.rem(lax.div(dp, 2), 2)
    mate = dp + 1 - 2 * core
    twin = dp + 2 - 4 * pair
    quad = 2 * pair + core
    quad_twin = 2 * (1 - pair) + core

    barrier = pltpu.get_barrier_semaphore()
    for to in ({"sp": right}, {"sp": left}, {"dp": mate}, {"dp": twin}):
        pl.semaphore_signal(barrier, inc=1, device_id=to, device_id_type=MESH)
    pl.semaphore_wait(barrier, 4)

    RIGHT, LEFT, MATE, TWIN = {"sp": right}, {"sp": left}, {"dp": mate}, {"dp": twin}

    class Kind:
        def __init__(self, buf, first, count, rows, cols, alone, sources):
            self.buf, self.first, self.count, self.cols, self.sources = buf, first, count, cols, sources
            shared = rows - alone
            self.shared, self.part, self.half = shared, shared // 4, alone // 2
            self.total = self.part + self.half

        def ranges(self, quad_index=None):
            got = [(pl.multiple_of(quad * self.part, 8), self.part)]
            if self.half:
                got.append((pl.multiple_of(self.shared + core * self.half, 8), self.half))
            return got

        def move(self, c, shard, at, size, to, group):
            view = self.buf.at[c, shard, pl.ds(at, size), :]
            pltpu.make_async_remote_copy(src_ref=view, dst_ref=view, send_sem=send.at[self.first + c, group],
                                         recv_sem=recv.at[self.first + c, group], device_id=to, device_id_type=MESH).start()

        def took(self, sems, c, group, rows):
            for at in range(0, rows, self.total):
                pass
            shards = 1
            while rows // shards > self.shared + 2 * self.half or rows % shards:
                shards += 1
            view = self.buf.at[c, pl.ds(0, shards), pl.ds(0, rows // shards), :]
            pltpu.make_async_copy(view, view, sems.at[self.first + c, group]).wait()

        def e0(self, c):
            for group, to in ((0, RIGHT), (1, LEFT)):
                for at, size in self.ranges():
                    for ref, col, place, cols in self.sources(c):
                        pltpu.make_async_remote_copy(
                            src_ref=ref.at[pl.ds(at, size), pl.ds(col, cols)],
                            dst_ref=self.buf.at[c, me, pl.ds(at, size), pl.ds(place, cols)],
                            send_sem=send.at[self.first + c, group], recv_sem=recv.at[self.first + c, group],
                            device_id=to, device_id_type=MESH).start()

        def e1(self, c):
            self.took(recv, c, 0, self.total)
            for at, size in self.ranges():
                self.move(c, left, at, size // 2, RIGHT, 2)
            self.took(recv, c, 1, self.total)
            for at, size in self.ranges():
                self.move(c, right, at + size // 2, size // 2, LEFT, 3)
            at, size = self.ranges()[0]
            for shard in (left, right):
                self.move(c, shard, at, size, TWIN, 4)
            for shard in (left, right):
                for at, size in self.ranges():
                    self.move(c, shard, at, size, MATE, 6)

        def e2(self, c):
            self.took(recv, c, 2, self.total // 2)
            self.took(recv, c, 3, self.total // 2)
            at, size = self.ranges()[0]
            self.move(c, across, at, size, TWIN, 5)
            for at, size in self.ranges():
                self.move(c, across, at, size, MATE, 7)

        def e3(self, c):
            at = pl.multiple_of(quad_twin * self.part, 8)
            self.took(recv, c, 4, 2 * self.part)
            self.took(recv, c, 5, self.part)
            for shard in (left, right, across):
                self.move(c, shard, at, self.part, MATE, 8)

        def e4(self, c):
            self.took(recv, c, 6, 2 * self.total)
            self.took(recv, c, 7, self.total)
            self.took(recv, c, 8, 3 * self.part)

        def sent(self, c):
            for group, rows in enumerate((self.total, self.total, self.total // 2, self.total // 2, 2 * self.part, self.part,
                                          2 * self.total, self.total, 3 * self.part)):
                self.took(send, c, group, rows)

    def sources_q(c):
        return ((wq_ref, pl.multiple_of(c * qcols, HEAD), 0, qcols), (wk_ref, pl.multiple_of(c * HEAD, HEAD), qcols, HEAD),
                (wv_ref, pl.multiple_of(c * HEAD, HEAD), qcols + HEAD, HEAD))

    def sources_o(c):
        return ((wo_ref, pl.multiple_of(c * WO_COLS, HEAD), 0, WO_COLS),)

    kq = Kind(gw_ref, 0, nq, rows_q, ccols, alone_q, sources_q)
    ko = Kind(go_ref, nq, no, rows_o, WO_COLS, alone_o, sources_o)

    def event(name, i):
        if isinstance(i, int):
            kind, c = (kq, i) if i < nq else (ko, i - nq)
            getattr(kind, name)(c)
            return

        @pl.when(i < nq)
        def _():
            getattr(kq, name)(i)

        @pl.when((i >= nq) & (i < nq + no))
        def _():
            getattr(ko, name)(i - nq)

    def forward(i):
        event("e1", i)
        event("e0", i + 1)

    def load_q(c):
        for step in range(1, n):
            shard = lax.rem(me + step, n)
            pltpu.make_async_copy(gw_ref.at[c, shard], w_s.at[pl.ds(pl.multiple_of(shard * rows_q, 8), rows_q), :], wl.at[0]).start()
        mine = pl.ds(pl.multiple_of(me * rows_q, 8), rows_q)
        for ref, col, place, cols in sources_q(c):
            pltpu.make_async_copy(ref.at[:, pl.ds(col, cols)], w_s.at[mine, pl.ds(place, cols)], wl.at[0]).start()

    def load_q_wait():
        pltpu.make_async_copy(w_s, w_s, wl.at[0]).wait()

    def load_o(c, half):
        cols = pl.ds(half * TILE, TILE)
        for step in range(1, n):
            shard = lax.rem(me + step, n)
            pltpu.make_async_copy(go_ref.at[c, shard, :, cols], w_s.at[pl.ds(pl.multiple_of(shard * rows_o, 8), rows_o), cols],
                                  wl.at[half]).start()
        place = pl.ds(pl.multiple_of(c * WO_COLS + half * TILE, HEAD), TILE)
        pltpu.make_async_copy(wo_ref.at[:, place], w_s.at[pl.ds(pl.multiple_of(me * rows_o, 8), rows_o), cols], wl.at[half]).start()
        pltpu.make_async_copy(x_ref.at[:, place], xr.at[half], xl.at[half]).start()

    def load_o_wait(half):
        view = w_s.at[pl.ds(0, n * rows_o), pl.ds(half * TILE, TILE)]
        pltpu.make_async_copy(view, view, wl.at[half]).wait()
        pltpu.make_async_copy(xr.at[half], xr.at[half], xl.at[half]).wait()

    def norm():
        def fetch(b, slot):
            return pltpu.make_async_copy(x_ref.at[pl.ds(pl.multiple_of(b * NORM_ROWS, 8), NORM_ROWS), :], xb.at[slot], rl.at[slot])

        blocks = own // NORM_ROWS
        fetch(0, 0).start()

        def body(b, _):
            slot = lax.rem(b, 2)

            @pl.when(b + 1 < blocks)
            def _():
                fetch(b + 1, 1 - slot).start()

            fetch(b, slot).wait()
            wide = xb[slot].astype(F32)
            scale = lax.rsqrt(jnp.mean(wide * wide, -1, keepdims=True) + 1e-6)
            a_s[pl.ds(pl.multiple_of(b * NORM_ROWS, 8), NORM_ROWS), :] = (wide * scale * gain_ref[...].astype(F32)).astype(BF16)

        lax.fori_loop(0, blocks, body, None)

    def project(slot):
        def tile(t, _):
            cols = pl.ds(pl.multiple_of(t * TILE, TILE), TILE)
            t_s[:, cols] = jnp.dot(a_s[...], w_s[:, cols], preferred_element_type=F32).astype(BF16)

        lax.fori_loop(0, ccols // TILE, tile, None)

        def turned(t):
            wide = t.astype(F32)
            return (wide * cos_ref[...] + pltpu.roll(wide, HEAD // 2, 1) * sin_ref[...]).astype(BF16)

        kst[slot] = turned(t_s[:, qcols : qcols + HEAD])
        vst[slot] = t_s[:, qcols + HEAD :].astype(F32).T.astype(BF16)
        for h in range(share):
            q_s[slot, h] = turned(t_s[:, h * HEAD : (h + 1) * HEAD])

    def kv_move(g, shard, k_src, v_src, to, s, r):
        for src, dst in ((k_src, kall_ref.at[g, shard]), (v_src, vall_ref.at[g, shard])):
            pltpu.make_async_remote_copy(src_ref=src, dst_ref=dst, send_sem=ksend.at[g, s], recv_sem=krecv.at[g, r],
                                         device_id=to, device_id_type=MESH).start()

    def kv_took(sem):
        view = kall_ref.at[0, pl.ds(0, 2)]
        pltpu.make_async_copy(view, view, sem).wait()

    def f1(g, slot):
        @pl.when(me < n - 1)
        def _():
            kv_move(g, me, kst.at[slot], vst.at[slot], RIGHT, 0, 0)

        @pl.when(me == 0)
        def _():
            kv_move(g, me, kst.at[slot], vst.at[slot], LEFT, 1, 1)

    def f2(g):
        @pl.when(me >= 1)
        def _():
            kv_took(krecv.at[g, 0])

        @pl.when(me == n - 2)
        def _():
            kv_move(g, left, kall_ref.at[g, left], vall_ref.at[g, left], RIGHT, 1, 2)

        @pl.when(me == n - 1)
        def _():
            kv_took(krecv.at[g, 1])
            kv_move(g, right, kall_ref.at[g, right], vall_ref.at[g, right], LEFT, 1, 2)

    def f3(g):
        @pl.when(me >= n - 2)
        def _():
            kv_took(krecv.at[g, 2])

    def kv_sent(g):
        @pl.when(me < n - 1)
        def _():
            kv_took(ksend.at[g, 0])

        @pl.when((me == 0) | (me >= n - 2))
        def _():
            kv_took(ksend.at[g, 1])

    def kv_load(g, slot):
        def copies(j, k_src, v_src):
            return (pltpu.make_async_copy(k_src, k_s.at[pl.ds(pl.multiple_of(j * own, own), own), :], kl.at[j]),
                    pltpu.make_async_copy(v_src, v_s.at[pl.ds(0, HEAD), pl.ds(pl.multiple_of(j * own, own), own)], kl.at[j]))

        for c in copies(me, kst.at[slot], vst.at[slot]):
            c.start()
        for j in range(n):
            @pl.when(j < me)
            def _():
                for c in copies(j, kall_ref.at[g, j], vall_ref.at[g, j]):
                    c.start()

        view = k_s.at[pl.ds(0, 2 * own), :]
        for j in range(n):
            @pl.when(j <= me)
            def _():
                pltpu.make_async_copy(view, view, kl.at[j]).wait()

    per = own // STRIP
    scale = HEAD**-0.5
    e = scale * LOG2E

    def block(slot, j, strips, masked):
        here = pl.ds(pl.multiple_of(j * STRIP, STRIP), STRIP)
        keys, values = k_s[here, :], v_s[:, here]
        scores = [_dot(keys, q_s[slot, s % share, (s // share) * STRIP : (s // share + 1) * STRIP, :], 1, 1) for s in strips]
        weights, keeps = [], []
        if masked:
            ok = lax.broadcasted_iota(jnp.int32, (STRIP, STRIP), 0) <= lax.broadcasted_iota(jnp.int32, (STRIP, STRIP), 1)
        for s, score in zip(strips, scores):
            if s in masked:
                score = jnp.where(ok, score, HIDDEN)
            old = top_s[s : s + 1, :]
            top = jnp.maximum(old, score.max(axis=0, keepdims=True))
            top_s[s : s + 1, :] = top
            weights.append(jnp.exp2((score - top) * e).astype(BF16))
            keeps.append(jnp.exp2((old - top) * e))
        for s, p, keep in zip(strips, weights, keeps):
            at = slice(s * STRIP, (s + 1) * STRIP)
            mix_s[:, at] = mix_s[:, at] * keep + _dot(values, p, 1, 0)

    def attend(g, slot):
        strips = list(range(per * share))
        top_s[...] = jnp.full(top_s.shape, NEG, F32)
        mix_s[...] = jnp.zeros(mix_s.shape, F32)
        lax.fori_loop(0, per * me, lambda j, _: block(slot, j, strips, ()), None)
        for d in range(per):
            block(slot, per * me + d, strips[d * share :], strips[d * share : (d + 1) * share])
        for s in strips:
            at = slice(s * STRIP, (s + 1) * STRIP)
            out = (mix_s[:HEAD, at] * (1 / mix_s[HEAD : HEAD + 1, at])).T
            seen_s[(s // share) * STRIP : (s // share + 1) * STRIP,
                   pl.ds(pl.multiple_of(g * qcols + (s % share) * HEAD, HEAD), HEAD)] = out.astype(BF16)

    event("e0", 0)
    v_s[HEAD:, :] = jnp.ones((8, n * own), BF16)
    norm()
    forward(0)
    event("e2", 0)
    forward(1)
    event("e3", 0)
    event("e2", 1)
    event("e4", 0)
    load_q(0)
    forward(2)
    event("e2", 2)

    def group(it, _):
        slot = lax.rem(it, 2)

        @pl.when(it >= 1)
        def _():
            f2(it - 1)

        @pl.when(it < groups)
        def _():
            event("e3", it + 1)

            @pl.when(it >= 2)
            def _():
                kv_sent(it - 2)

            load_q_wait()
            project(slot)
            f1(it, slot)
            event("e4", it + 1)

            @pl.when(it + 1 < groups)
            def _():
                load_q(it + 1)

        forward(it + 3)

        @pl.when(it >= 1)
        def _():
            f3(it - 1)
            kv_load(it - 1, 1 - slot)
            attend(it - 1, 1 - slot)

        event("e2", it + 3)

    lax.fori_loop(0, groups + 1, group, None)

    def put(c, half):
        return pltpu.make_async_copy(yb.at[half], y_ref.at[:, pl.ds(pl.multiple_of(c * WO_COLS + half * TILE, HEAD), TILE)], yl.at[half])

    load_o(0, 0)

    def last(c, _):
        forward(nq + c + 4)
        for half in range(WO_COLS // TILE):
            if half == 0:
                load_o(c, 1)
            load_o_wait(half)

            @pl.when(c >= 1)
            def _():
                put(c - 1, half).wait()

            cols = pl.ds(half * TILE, TILE)
            y = jnp.dot(seen_s[...], w_s[: n * rows_o, half * TILE : (half + 1) * TILE], preferred_element_type=F32)
            yb[half] = (xr[half].astype(F32) + y).astype(BF16)
            put(c, half).start()
        event("e2", nq + c + 4)

        @pl.when(c + 1 < no)
        def _():
            event("e3", nq + c + 1)
            event("e4", nq + c + 1)
            load_o(c + 1, 0)

    lax.fori_loop(0, no, last, None)
    for half in range(WO_COLS // TILE):
        put(no - 1, half).wait()
    kv_sent(groups - 2)
    kv_sent(groups - 1)
    lax.fori_loop(0, nq, lambda c, _: kq.sent(c), None)
    lax.fori_loop(0, no, lambda c, _: ko.sent(c), None)


def solution(mesh):
    n = mesh.shape["sp"]

    def step(x, gain, wq, wk, wv, wo):
        own, width = x.shape
        groups, share = wk.shape[1] // HEAD, wq.shape[1] // wk.shape[1]
        heads = groups * share
        nq, no = groups, width // WO_COLS
        ccols = (share + 2) * HEAD
        rows_q, rows_o = wq.shape[0], wo.shape[0]
        place = lax.axis_index("sp") * own + jnp.arange(own)
        angle = place.astype(F32)[:, None] * THETA ** (-jnp.arange(HEAD // 2, dtype=F32) / (HEAD // 2))
        cos, sin = jnp.cos(angle), jnp.sin(angle)
        cos, sin = jnp.concatenate([cos, cos], -1), jnp.concatenate([-sin, sin], -1)
        hbm, vmem = pl.BlockSpec(memory_space=pl.ANY), pl.BlockSpec(memory_space=pltpu.VMEM)
        dims = (n, groups, share, nq, no, 0, 0)
        dma = pltpu.SemaphoreType.DMA
        got = pl.pallas_call(
            functools.partial(kernel, dims),
            in_specs=[hbm, vmem, vmem, vmem, hbm, hbm, hbm, hbm],
            out_specs=[hbm] * 5,
            out_shape=[jax.ShapeDtypeStruct(s, BF16) for s in (
                (own, width), (nq, n, rows_q, ccols), (no, n, rows_o, WO_COLS), (groups, n, own, HEAD), (groups, n, HEAD, own))],
            scratch_shapes=[
                pltpu.VMEM((own, width), BF16),
                pltpu.VMEM((width, ccols), BF16),
                pltpu.VMEM((own, ccols), BF16),
                pltpu.VMEM((2, share, own, HEAD), BF16),
                pltpu.VMEM((2, own, HEAD), BF16),
                pltpu.VMEM((2, HEAD, own), BF16),
                pltpu.VMEM((n * own, HEAD), BF16),
                pltpu.VMEM((HEAD + 8, n * own), BF16),
                pltpu.VMEM((own, heads * HEAD), BF16),
                pltpu.VMEM((own * share // STRIP, STRIP), F32),
                pltpu.VMEM((HEAD + 8, own * share), F32),
                pltpu.VMEM((2, NORM_ROWS, width), BF16),
                pltpu.VMEM((2, own, TILE), BF16),
                pltpu.VMEM((2, own, TILE), BF16),
                dma((nq + no, 9)), dma((nq + no, 9)), dma((groups, 2)), dma((groups, 3)),
                dma((2,)), dma((n,)), dma((2,)), dma((2,)), dma((2,)),
            ],
            compiler_params=pltpu.CompilerParams(collective_id=0, has_side_effects=True, vmem_limit_bytes=VMEM),
            cost_estimate=pl.CostEstimate(flops=2 * own * width * (wq.shape[1] * 2 + wk.shape[1] * 2) + 4 * own * own * n * heads * HEAD,
                                          transcendentals=own * own * n * heads, bytes_accessed=2**28),
        )(x, gain[None], cos, sin, wq, wk, wv, wo)
        return got[0]

    tokens, whole = P(("dp", "sp"), None), P("sp", None)
    return jax.shard_map(step, mesh=mesh, in_specs=(tokens, P(None), whole, whole, whole, whole), out_specs=tokens, check_vma=False)
```

```python
import functools

import jax
import jax.numpy as jnp
from jax import lax
from jax.experimental import pallas as pl
from jax.experimental.pallas import tpu as pltpu
from jax.sharding import PartitionSpec as P

NEG = -1e30
HIDDEN = 2 * NEG
LOG2E = 1.4426950408889634
VMEM = 67043328
HEAD = 128
THETA = 10000
STRIP = 512
WO_COLS = 512
EARLY = 2
ALONE_EARLY = 448
ALONE_Q = 0
ALONE_O = 320
TILE = 256
NORM_ROWS = 128
MESH = pl.DeviceIdType.MESH
F32, BF16 = jnp.float32, jnp.bfloat16


def _dot(a, b, ca, cb):
    return lax.dot_general(a, b, (((ca,), (cb,)), ((), ())), preferred_element_type=F32)


def kernel(dims, x_ref, gain_ref, cos_ref, sin_ref, wq_ref, wk_ref, wv_ref, wo_ref,
           y_ref, gw_ref, go_ref, kall_ref, vall_ref,
           a_s, w_s, t_s, q_s, kst, vst, k_s, v_s, seen_s, top_s, mix_s, xb, xr, yb,
           send, recv, ksend, krecv, wl, ol, kl, xl, rl, yl):
    n, groups, share, nq, no = dims
    own, width = x_ref.shape
    rows_q, rows_o = wq_ref.shape[0], wo_ref.shape[0]
    qcols = share * HEAD
    ccols = qcols + 2 * HEAD
    me, dp = lax.axis_index("sp"), lax.axis_index("dp")
    right, left = lax.rem(me + 1, n), lax.rem(me + n - 1, n)
    across = lax.rem(me + 2, n)
    core, pair = lax.rem(dp, 2), lax.rem(lax.div(dp, 2), 2)
    mate = dp + 1 - 2 * core
    twin = dp + 2 - 4 * pair
    quad = 2 * pair + core
    quad_twin = 2 * (1 - pair) + core

    barrier = pltpu.get_barrier_semaphore()
    for to in ({"sp": right}, {"sp": left}, {"dp": mate}, {"dp": twin}):
        pl.semaphore_signal(barrier, inc=1, device_id=to, device_id_type=MESH)
    pl.semaphore_wait(barrier, 4)

    RIGHT, LEFT, MATE, TWIN = {"sp": right}, {"sp": left}, {"dp": mate}, {"dp": twin}

    class Kind:
        def __init__(self, buf, first, count, rows, cols, alone, sources):
            self.buf, self.first, self.count, self.cols, self.sources = buf, first, count, cols, sources
            shared = rows - alone
            self.shared, self.part, self.half = shared, shared // 4, alone // 2
            self.total = self.part + self.half

        def ranges(self, quad_index=None):
            got = [(pl.multiple_of(quad * self.part, 8), self.part)]
            if self.half:
                got.append((pl.multiple_of(self.shared + core * self.half, 8), self.half))
            return got

        def move(self, c, shard, at, size, to, group):
            view = self.buf.at[c, shard, pl.ds(at, size), :]
            pltpu.make_async_remote_copy(src_ref=view, dst_ref=view, send_sem=send.at[self.first + c, group],
                                         recv_sem=recv.at[self.first + c, group], device_id=to, device_id_type=MESH).start()

        def took(self, sems, c, group, rows):
            shards = 1
            while rows // shards > self.shared + 2 * self.half or rows % shards:
                shards += 1
            view = self.buf.at[c, pl.ds(0, shards), pl.ds(0, rows // shards), :]
            pltpu.make_async_copy(view, view, sems.at[self.first + c, group]).wait()

        def e0(self, c):
            for group, to in ((0, RIGHT), (1, LEFT)):
                for at, size in self.ranges():
                    for ref, col, place, cols in self.sources(c):
                        pltpu.make_async_remote_copy(
                            src_ref=ref.at[pl.ds(at, size), pl.ds(col, cols)],
                            dst_ref=self.buf.at[c, me, pl.ds(at, size), pl.ds(place, cols)],
                            send_sem=send.at[self.first + c, group], recv_sem=recv.at[self.first + c, group],
                            device_id=to, device_id_type=MESH).start()

        def e1(self, c):
            self.took(recv, c, 0, self.total)
            for at, size in self.ranges():
                self.move(c, left, at, size // 2, RIGHT, 2)
            self.took(recv, c, 1, self.total)
            for at, size in self.ranges():
                self.move(c, right, at + size // 2, size // 2, LEFT, 3)
            at, size = self.ranges()[0]
            for shard in (left, right):
                self.move(c, shard, at, size, TWIN, 4)
            for shard in (left, right):
                for at, size in self.ranges():
                    self.move(c, shard, at, size, MATE, 6)

        def e2(self, c):
            self.took(recv, c, 2, self.total // 2)
            self.took(recv, c, 3, self.total // 2)
            at, size = self.ranges()[0]
            self.move(c, across, at, size, TWIN, 5)
            for at, size in self.ranges():
                self.move(c, across, at, size, MATE, 7)

        def e3(self, c):
            at = pl.multiple_of(quad_twin * self.part, 8)
            self.took(recv, c, 4, 2 * self.part)
            self.took(recv, c, 5, self.part)
            for shard in (left, right, across):
                self.move(c, shard, at, self.part, MATE, 8)

        def e4(self, c):
            self.took(recv, c, 6, 2 * self.total)
            self.took(recv, c, 7, self.total)
            self.took(recv, c, 8, 3 * self.part)

        def sent(self, c):
            for group, rows in enumerate((self.total, self.total, self.total // 2, self.total // 2, 2 * self.part, self.part,
                                          2 * self.total, self.total, 3 * self.part)):
                self.took(send, c, group, rows)

    def sources_q(c):
        return ((wq_ref, pl.multiple_of(c * qcols, HEAD), 0, qcols), (wk_ref, pl.multiple_of(c * HEAD, HEAD), qcols, HEAD),
                (wv_ref, pl.multiple_of(c * HEAD, HEAD), qcols + HEAD, HEAD))

    def sources_o(c):
        return ((wo_ref, pl.multiple_of(c * WO_COLS, HEAD), 0, WO_COLS),)

    kf = Kind(gw_ref, 0, nq, rows_q, ccols, ALONE_EARLY, sources_q)
    kq = Kind(gw_ref, 0, nq, rows_q, ccols, ALONE_Q, sources_q)
    ko = Kind(go_ref, nq, no, rows_o, WO_COLS, ALONE_O, sources_o)

    def event(name, i, early=False):
        if isinstance(i, int):
            getattr(kf if i < EARLY else kq, name)(i)
            return
        if early:
            @pl.when(i < EARLY)
            def _():
                getattr(kf, name)(i)

        @pl.when((i >= EARLY) & (i < nq))
        def _():
            getattr(kq, name)(i)

    def event_o(name, i):
        @pl.when((i >= 0) & (i < no))
        def _():
            getattr(ko, name)(i)

    def forward(i):
        event("e1", i)
        event("e0", i + 1)

    def forward_o(i):
        event_o("e1", i)
        event_o("e0", i + 1)

    def load_q(c):
        for step in range(1, n):
            shard = lax.rem(me + step, n)
            pltpu.make_async_copy(gw_ref.at[c, shard], w_s.at[pl.ds(pl.multiple_of(shard * rows_q, 8), rows_q), :], wl.at[0]).start()
        mine = pl.ds(pl.multiple_of(me * rows_q, 8), rows_q)
        for ref, col, place, cols in sources_q(c):
            pltpu.make_async_copy(ref.at[:, pl.ds(col, cols)], w_s.at[mine, pl.ds(place, cols)], wl.at[0]).start()

    def load_q_wait():
        pltpu.make_async_copy(w_s, w_s, wl.at[0]).wait()

    def load_o(s):
        c, half, slot = lax.div(s, 2), lax.rem(s, 2), lax.rem(s, 3)
        cols, to = pl.ds(pl.multiple_of(half * TILE, TILE), TILE), pl.ds(pl.multiple_of(slot * TILE, TILE), TILE)
        for step in range(1, n):
            shard = lax.rem(me + step, n)
            pltpu.make_async_copy(go_ref.at[c, shard, :, cols], w_s.at[pl.ds(pl.multiple_of(shard * rows_o, 8), rows_o), to],
                                  ol.at[slot]).start()
        place = pl.ds(pl.multiple_of(s * TILE, TILE), TILE)
        pltpu.make_async_copy(wo_ref.at[:, place], w_s.at[pl.ds(pl.multiple_of(me * rows_o, 8), rows_o), to], ol.at[slot]).start()
        pltpu.make_async_copy(x_ref.at[:, place], xr.at[slot], xl.at[slot]).start()

    def load_o_wait(slot):
        view = w_s.at[pl.ds(0, n * rows_o), pl.ds(0, TILE)]
        pltpu.make_async_copy(view, view, ol.at[slot]).wait()
        pltpu.make_async_copy(xr.at[0], xr.at[0], xl.at[slot]).wait()

    def norm():
        def fetch(b, slot):
            return pltpu.make_async_copy(x_ref.at[pl.ds(pl.multiple_of(b * NORM_ROWS, 8), NORM_ROWS), :], xb.at[slot], rl.at[slot])

        blocks = own // NORM_ROWS
        fetch(0, 0).start()

        def body(b, _):
            slot = lax.rem(b, 2)

            @pl.when(b + 1 < blocks)
            def _():
                fetch(b + 1, 1 - slot).start()

            fetch(b, slot).wait()
            wide = xb[slot].astype(F32)
            scale = lax.rsqrt(jnp.mean(wide * wide, -1, keepdims=True) + 1e-6)
            a_s[pl.ds(pl.multiple_of(b * NORM_ROWS, 8), NORM_ROWS), :] = (wide * scale * gain_ref[...].astype(F32)).astype(BF16)

        lax.fori_loop(0, blocks, body, None)

    def project(slot):
        def tile(t, _):
            cols = pl.ds(pl.multiple_of(t * TILE, TILE), TILE)
            t_s[:, cols] = jnp.dot(a_s[...], w_s[:, cols], preferred_element_type=F32).astype(BF16)

        lax.fori_loop(0, ccols // TILE, tile, None)

        def turned(t):
            wide = t.astype(F32)
            return (wide * cos_ref[...] + pltpu.roll(wide, HEAD // 2, 1) * sin_ref[...]).astype(BF16)

        kst[slot] = turned(t_s[:, qcols : qcols + HEAD])
        vst[slot] = t_s[:, qcols + HEAD :].astype(F32).T.astype(BF16)
        for h in range(share):
            q_s[slot, h] = turned(t_s[:, h * HEAD : (h + 1) * HEAD])

    def keys_move(g, shard, src, to, s, r):
        pltpu.make_async_remote_copy(src_ref=src, dst_ref=kall_ref.at[g, shard], send_sem=ksend.at[g, s], recv_sem=krecv.at[g, r],
                                     device_id=to, device_id_type=MESH).start()

    def values_move(g, shard, src, to, s, r):
        pltpu.make_async_remote_copy(src_ref=src, dst_ref=vall_ref.at[g, shard], send_sem=ksend.at[g, s], recv_sem=krecv.at[g, r],
                                     device_id=to, device_id_type=MESH).start()

    def kv_took(sem, arrays=2):
        view = kall_ref.at[0, pl.ds(0, arrays)]
        pltpu.make_async_copy(view, view, sem).wait()

    def f1(g, slot):
        @pl.when(me < n - 1)
        def _():
            keys_move(g, me, kst.at[slot], RIGHT, 0, 0)
            values_move(g, me, vst.at[slot], RIGHT, 0, 0)

        @pl.when(me == 0)
        def _():
            keys_move(g, me, kst.at[slot], LEFT, 1, 1)
            values_move(g, me, vst.at[slot], LEFT, 1, 1)

        @pl.when(me == 1)
        def _():
            values_move(g, me, vst.at[slot], LEFT, 1, 0)

    def f2(g):
        @pl.when(me == 0)
        def _():
            kv_took(krecv.at[g, 0], 1)
            values_move(g, right, vall_ref.at[g, right], LEFT, 2, 3)

        @pl.when(me >= 1)
        def _():
            kv_took(krecv.at[g, 0])

        @pl.when(me == n - 2)
        def _():
            keys_move(g, left, kall_ref.at[g, left], RIGHT, 1, 2)

        @pl.when(me == n - 1)
        def _():
            kv_took(krecv.at[g, 1])
            keys_move(g, right, kall_ref.at[g, right], LEFT, 1, 2)
            values_move(g, right, vall_ref.at[g, right], LEFT, 1, 2)

    def f3(g):
        @pl.when(me == n - 2)
        def _():
            kv_took(krecv.at[g, 2])

        @pl.when(me == n - 1)
        def _():
            kv_took(krecv.at[g, 2], 1)
            kv_took(krecv.at[g, 3], 1)

    def kv_sent(g):
        @pl.when(me < n - 1)
        def _():
            kv_took(ksend.at[g, 0])

        @pl.when((me == 0) | (me == n - 1))
        def _():
            kv_took(ksend.at[g, 1])

        @pl.when((me == 1) | (me == n - 2))
        def _():
            kv_took(ksend.at[g, 1], 1)

        @pl.when(me == 0)
        def _():
            kv_took(ksend.at[g, 2], 1)

    def kv_copy(j, k_src, v_src):
        here = pl.ds(pl.multiple_of(j * own, own), own)
        pltpu.make_async_copy(k_src, k_s.at[here, :], kl.at[j]).start()
        pltpu.make_async_copy(v_src, v_s.at[pl.ds(0, HEAD), here], kl.at[j]).start()

    def kv_early(g, slot):
        kv_copy(me, kst.at[slot], vst.at[slot])

        @pl.when(me >= 1)
        def _():
            kv_copy(left, kall_ref.at[g, left], vall_ref.at[g, left])

        @pl.when(me == n - 1)
        def _():
            kv_copy(right, kall_ref.at[g, right], vall_ref.at[g, right])

    def kv_late(g):
        @pl.when(me >= n - 2)
        def _():
            kv_copy(across, kall_ref.at[g, across], vall_ref.at[g, across])

    def kv_wait():
        view = k_s.at[pl.ds(0, 2 * own), :]
        for j in range(n):
            @pl.when(j <= me)
            def _():
                pltpu.make_async_copy(view, view, kl.at[j]).wait()

    per = own // STRIP
    scale = HEAD**-0.5
    e = scale * LOG2E

    def block(slot, j, strips, masked):
        here = pl.ds(pl.multiple_of(j * STRIP, STRIP), STRIP)
        keys, values = k_s[here, :], v_s[:, here]
        scores = [_dot(keys, q_s[slot, s % share, (s // share) * STRIP : (s // share + 1) * STRIP, :], 1, 1) for s in strips]
        weights, keeps = [], []
        if masked:
            ok = lax.broadcasted_iota(jnp.int32, (STRIP, STRIP), 0) <= lax.broadcasted_iota(jnp.int32, (STRIP, STRIP), 1)
        for s, score in zip(strips, scores):
            if s in masked:
                score = jnp.where(ok, score, HIDDEN)
            old = top_s[s : s + 1, :]
            top = jnp.maximum(old, score.max(axis=0, keepdims=True))
            top_s[s : s + 1, :] = top
            weights.append(jnp.exp2((score - top) * e).astype(BF16))
            keeps.append(jnp.exp2((old - top) * e))
        for s, p, keep in zip(strips, weights, keeps):
            at = slice(s * STRIP, (s + 1) * STRIP)
            mix_s[:, at] = mix_s[:, at] * keep + _dot(values, p, 1, 0)

    strips = list(range(per * share))

    def attend(slot):
        top_s[...] = jnp.full(top_s.shape, NEG, F32)
        mix_s[...] = jnp.zeros(mix_s.shape, F32)
        lax.fori_loop(0, per * me, lambda j, _: block(slot, j, strips, ()), None)

    def attend_end(g, slot):
        for d in range(per):
            block(slot, per * me + d, strips[d * share :], strips[d * share : (d + 1) * share])
        for s in strips:
            at = slice(s * STRIP, (s + 1) * STRIP)
            out = (mix_s[:HEAD, at] * (1 / mix_s[HEAD : HEAD + 1, at])).T
            seen_s[(s // share) * STRIP : (s // share + 1) * STRIP,
                   pl.ds(pl.multiple_of(g * qcols + (s % share) * HEAD, HEAD), HEAD)] = out.astype(BF16)

    event("e0", 0)
    v_s[HEAD:, :] = jnp.ones((8, n * own), BF16)
    norm()
    forward(0)
    event("e2", 0)
    forward(1)
    event("e3", 0)
    event("e2", 1)
    event("e4", 0)
    load_q(0)
    forward(2)
    event("e2", 2)

    def group(it, _):
        slot = lax.rem(it, 2)
        first_o = it - 1 + lax.div(it, groups)

        @pl.when(it >= 1)
        def _():
            f2(it - 1)
            kv_early(it - 1, 1 - slot)

        @pl.when(it < groups)
        def _():
            @pl.when(it >= 2)
            def _():
                kv_sent(it - 2)

            load_q_wait()
            project(slot)
            f1(it, slot)
            event("e3", it + 1, True)

        @pl.when(it == groups)
        def _():
            load_o(0)
            load_o(1)

        forward(it + 3)
        event_o("e3", it - 3)
        forward_o(first_o)

        @pl.when(it >= groups - 1)
        def _():
            forward_o(first_o + 1)

        @pl.when(it >= 1)
        def _():
            f3(it - 1)
            kv_late(it - 1)
            kv_wait()
            attend(1 - slot)

        @pl.when(it + 1 < groups)
        def _():
            event("e4", it + 1, True)
            load_q(it + 1)

        event_o("e4", it - 3)

        @pl.when(it >= 1)
        def _():
            attend_end(it - 1, 1 - slot)

        event("e2", it + 3)
        event_o("e2", first_o)

        @pl.when(it >= groups - 1)
        def _():
            event_o("e2", first_o + 1)

    lax.fori_loop(0, groups + 1, group, None)

    def put(s):
        half = lax.rem(s, 2)
        return pltpu.make_async_copy(yb.at[half], y_ref.at[:, pl.ds(pl.multiple_of(s * TILE, TILE), TILE)], yl.at[half])

    pieces = width // TILE

    def last(s, _):
        c, half, slot = lax.div(s, 2), lax.rem(s, 2), lax.rem(s, 3)

        @pl.when(half == 0)
        def _():
            event_o("e3", c + groups - 2)

        @pl.when(s + 2 < pieces)
        def _():
            load_o(s + 2)

        load_o_wait(slot)

        @pl.when(s >= 2)
        def _():
            put(s - 2).wait()

        y = jnp.dot(seen_s[...], w_s[: n * rows_o, pl.ds(pl.multiple_of(slot * TILE, TILE), TILE)], preferred_element_type=F32)
        yb[half] = (xr[slot].astype(F32) + y).astype(BF16)
        put(s).start()

        @pl.when(half == 1)
        def _():
            event_o("e4", c + groups - 2)

    lax.fori_loop(0, pieces, last, None)
    put(pieces - 2).wait()
    put(pieces - 1).wait()
    kv_sent(groups - 2)
    kv_sent(groups - 1)
    for c in range(EARLY):
        kf.sent(c)
    lax.fori_loop(EARLY, nq, lambda c, _: kq.sent(c), None)
    lax.fori_loop(0, no, lambda c, _: ko.sent(c), None)


def solution(mesh):
    n = mesh.shape["sp"]

    def step(x, gain, wq, wk, wv, wo):
        own, width = x.shape
        groups, share = wk.shape[1] // HEAD, wq.shape[1] // wk.shape[1]
        heads = groups * share
        nq, no = groups, width // WO_COLS
        ccols = (share + 2) * HEAD
        rows_q, rows_o = wq.shape[0], wo.shape[0]
        place = lax.axis_index("sp") * own + jnp.arange(own)
        angle = place.astype(F32)[:, None] * THETA ** (-jnp.arange(HEAD // 2, dtype=F32) / (HEAD // 2))
        cos, sin = jnp.cos(angle), jnp.sin(angle)
        cos, sin = jnp.concatenate([cos, cos], -1), jnp.concatenate([-sin, sin], -1)
        hbm, vmem = pl.BlockSpec(memory_space=pl.ANY), pl.BlockSpec(memory_space=pltpu.VMEM)
        dims = (n, groups, share, nq, no)
        dma = pltpu.SemaphoreType.DMA
        got = pl.pallas_call(
            functools.partial(kernel, dims),
            in_specs=[hbm, vmem, vmem, vmem, hbm, hbm, hbm, hbm],
            out_specs=[hbm] * 5,
            out_shape=[jax.ShapeDtypeStruct(s, BF16) for s in (
                (own, width), (nq, n, rows_q, ccols), (no, n, rows_o, WO_COLS), (groups, n, own, HEAD), (groups, n, HEAD, own))],
            scratch_shapes=[
                pltpu.VMEM((own, width), BF16),
                pltpu.VMEM((width, ccols), BF16),
                pltpu.VMEM((own, ccols), BF16),
                pltpu.VMEM((2, share, own, HEAD), BF16),
                pltpu.VMEM((2, own, HEAD), BF16),
                pltpu.VMEM((2, HEAD, own), BF16),
                pltpu.VMEM((n * own, HEAD), BF16),
                pltpu.VMEM((HEAD + 8, n * own), BF16),
                pltpu.VMEM((own, heads * HEAD), BF16),
                pltpu.VMEM((own * share // STRIP, STRIP), F32),
                pltpu.VMEM((HEAD + 8, own * share), F32),
                pltpu.VMEM((2, NORM_ROWS, width), BF16),
                pltpu.VMEM((3, own, TILE), BF16),
                pltpu.VMEM((2, own, TILE), BF16),
                dma((nq + no, 9)), dma((nq + no, 9)), dma((groups, 3)), dma((groups, 4)),
                dma((1,)), dma((3,)), dma((n,)), dma((3,)), dma((2,)), dma((2,)),
            ],
            compiler_params=pltpu.CompilerParams(collective_id=0, has_side_effects=True, vmem_limit_bytes=VMEM),
            cost_estimate=pl.CostEstimate(flops=2 * own * width * (wq.shape[1] * 2 + wk.shape[1] * 2) + 4 * own * own * n * heads * HEAD,
                                          transcendentals=own * own * n * heads, bytes_accessed=2**28),
        )(x, gain[None], cos, sin, wq, wk, wv, wo)
        return got[0]

    tokens, whole = P(("dp", "sp"), None), P("sp", None)
    return jax.shard_map(step, mesh=mesh, in_specs=(tokens, P(None), whole, whole, whole, whole), out_specs=tokens, check_vma=False)
```

```python
import functools

import jax
import jax.numpy as jnp
from jax import lax
from jax.experimental import pallas as pl
from jax.experimental.pallas import tpu as pltpu
from jax.sharding import PartitionSpec as P

NEG = -1e30
HIDDEN = 2 * NEG
LOG2E = 1.4426950408889634
VMEM = 67043328
HEAD = 128
THETA = 10000
STRIP = 512
WO_COLS = 512
EARLY = 2
ALONE_EARLY = 448
ALONE_Q = 0
ALONE_O = 0
BACK = 3
TILE = 256
NORM_ROWS = 128
MESH = pl.DeviceIdType.MESH
F32, BF16 = jnp.float32, jnp.bfloat16


def _dot(a, b, ca, cb):
    return lax.dot_general(a, b, (((ca,), (cb,)), ((), ())), preferred_element_type=F32)


def kernel(dims, x_ref, gain_ref, cos_ref, sin_ref, wq_ref, wk_ref, wv_ref, wo_ref,
           y_ref, gw_ref, go_ref, kall_ref, vall_ref,
           a_s, w_s, t_s, q_s, kst, vst, k_s, v_s, seen_s, top_s, mix_s, xb, xr, yb,
           send, recv, ksend, krecv, wl, ol, kl, xl, rl, yl):
    n, groups, share, nq, no = dims
    own, width = x_ref.shape
    rows_q, rows_o = wq_ref.shape[0], wo_ref.shape[0]
    qcols = share * HEAD
    ccols = qcols + 2 * HEAD
    me, dp = lax.axis_index("sp"), lax.axis_index("dp")
    right, left = lax.rem(me + 1, n), lax.rem(me + n - 1, n)
    across = lax.rem(me + 2, n)
    core, pair = lax.rem(dp, 2), lax.rem(lax.div(dp, 2), 2)
    mate = dp + 1 - 2 * core
    twin = dp + 2 - 4 * pair
    quad = 2 * pair + core
    quad_twin = 2 * (1 - pair) + core

    barrier = pltpu.get_barrier_semaphore()
    for to in ({"sp": right}, {"sp": left}, {"dp": mate}, {"dp": twin}):
        pl.semaphore_signal(barrier, inc=1, device_id=to, device_id_type=MESH)
    pl.semaphore_wait(barrier, 4)

    RIGHT, LEFT, MATE, TWIN = {"sp": right}, {"sp": left}, {"dp": mate}, {"dp": twin}

    class Kind:
        def __init__(self, buf, first, count, rows, cols, alone, sources):
            self.buf, self.first, self.count, self.cols, self.sources = buf, first, count, cols, sources
            shared = rows - alone
            self.shared, self.part, self.half = shared, shared // 4, alone // 2
            self.total = self.part + self.half

        def ranges(self, quad_index=None):
            got = [(pl.multiple_of(quad * self.part, 8), self.part)]
            if self.half:
                got.append((pl.multiple_of(self.shared + core * self.half, 8), self.half))
            return got

        def move(self, c, shard, at, size, to, group):
            view = self.buf.at[c, shard, pl.ds(at, size), :]
            pltpu.make_async_remote_copy(src_ref=view, dst_ref=view, send_sem=send.at[self.first + c, group],
                                         recv_sem=recv.at[self.first + c, group], device_id=to, device_id_type=MESH).start()

        def took(self, sems, c, group, rows):
            shards = 1
            while rows // shards > self.shared + 2 * self.half or rows % shards:
                shards += 1
            view = self.buf.at[c, pl.ds(0, shards), pl.ds(0, rows // shards), :]
            pltpu.make_async_copy(view, view, sems.at[self.first + c, group]).wait()

        def e0(self, c):
            for group, to in ((0, RIGHT), (1, LEFT)):
                for at, size in self.ranges():
                    for ref, col, place, cols in self.sources(c):
                        pltpu.make_async_remote_copy(
                            src_ref=ref.at[pl.ds(at, size), pl.ds(col, cols)],
                            dst_ref=self.buf.at[c, me, pl.ds(at, size), pl.ds(place, cols)],
                            send_sem=send.at[self.first + c, group], recv_sem=recv.at[self.first + c, group],
                            device_id=to, device_id_type=MESH).start()

        def e1(self, c):
            self.took(recv, c, 0, self.total)
            for at, size in self.ranges():
                self.move(c, left, at, size // 2, RIGHT, 2)
            self.took(recv, c, 1, self.total)
            for at, size in self.ranges():
                self.move(c, right, at + size // 2, size // 2, LEFT, 3)
            at, size = self.ranges()[0]
            for shard in (left, right):
                self.move(c, shard, at, size, TWIN, 4)
            for shard in (left, right):
                for at, size in self.ranges():
                    self.move(c, shard, at, size, MATE, 6)

        def e2(self, c):
            self.took(recv, c, 2, self.total // 2)
            self.took(recv, c, 3, self.total // 2)
            at, size = self.ranges()[0]
            self.move(c, across, at, size, TWIN, 5)
            for at, size in self.ranges():
                self.move(c, across, at, size, MATE, 7)

        def e3(self, c):
            at = pl.multiple_of(quad_twin * self.part, 8)
            self.took(recv, c, 4, 2 * self.part)
            self.took(recv, c, 5, self.part)
            for shard in (left, right, across):
                self.move(c, shard, at, self.part, MATE, 8)

        def e4(self, c):
            self.took(recv, c, 6, 2 * self.total)
            self.took(recv, c, 7, self.total)
            self.took(recv, c, 8, 3 * self.part)

        def sent(self, c):
            for group, rows in enumerate((self.total, self.total, self.total // 2, self.total // 2, 2 * self.part, self.part,
                                          2 * self.total, self.total, 3 * self.part)):
                self.took(send, c, group, rows)

    def sources_q(c):
        return ((wq_ref, pl.multiple_of(c * qcols, HEAD), 0, qcols), (wk_ref, pl.multiple_of(c * HEAD, HEAD), qcols, HEAD),
                (wv_ref, pl.multiple_of(c * HEAD, HEAD), qcols + HEAD, HEAD))

    def sources_o(c):
        return ((wo_ref, pl.multiple_of(c * WO_COLS, HEAD), 0, WO_COLS),)

    kf = Kind(gw_ref, 0, nq, rows_q, ccols, ALONE_EARLY, sources_q)
    kq = Kind(gw_ref, 0, nq, rows_q, ccols, ALONE_Q, sources_q)
    ko = Kind(go_ref, nq, no, rows_o, WO_COLS, ALONE_O, sources_o)

    def event(name, i, early=False):
        if isinstance(i, int):
            getattr(kf if i < EARLY else kq, name)(i)
            return
        if early:
            @pl.when(i < EARLY)
            def _():
                getattr(kf, name)(i)

        @pl.when((i >= EARLY) & (i < nq))
        def _():
            getattr(kq, name)(i)

    def event_o(name, i):
        @pl.when((i >= 0) & (i < no))
        def _():
            getattr(ko, name)(i)

    def forward(i):
        event("e1", i)
        event("e0", i + 1)

    def forward_o(i):
        event_o("e1", i)
        event_o("e0", i + 1)

    def load_q(c):
        for step in range(1, n):
            shard = lax.rem(me + step, n)
            pltpu.make_async_copy(gw_ref.at[c, shard], w_s.at[pl.ds(pl.multiple_of(shard * rows_q, 8), rows_q), :], wl.at[0]).start()
        mine = pl.ds(pl.multiple_of(me * rows_q, 8), rows_q)
        for ref, col, place, cols in sources_q(c):
            pltpu.make_async_copy(ref.at[:, pl.ds(col, cols)], w_s.at[mine, pl.ds(place, cols)], wl.at[0]).start()

    def load_q_wait():
        pltpu.make_async_copy(w_s, w_s, wl.at[0]).wait()

    def load_o(s):
        c, half, slot = lax.div(s, 2), lax.rem(s, 2), lax.rem(s, 3)
        cols, to = pl.ds(pl.multiple_of(half * TILE, TILE), TILE), pl.ds(pl.multiple_of(slot * TILE, TILE), TILE)
        for step in range(1, n):
            shard = lax.rem(me + step, n)
            pltpu.make_async_copy(go_ref.at[c, shard, :, cols], w_s.at[pl.ds(pl.multiple_of(shard * rows_o, 8), rows_o), to],
                                  ol.at[slot]).start()
        place = pl.ds(pl.multiple_of(s * TILE, TILE), TILE)
        pltpu.make_async_copy(wo_ref.at[:, place], w_s.at[pl.ds(pl.multiple_of(me * rows_o, 8), rows_o), to], ol.at[slot]).start()
        pltpu.make_async_copy(x_ref.at[:, place], xr.at[slot], xl.at[slot]).start()

    def load_o_wait(slot):
        view = w_s.at[pl.ds(0, n * rows_o), pl.ds(0, TILE)]
        pltpu.make_async_copy(view, view, ol.at[slot]).wait()
        pltpu.make_async_copy(xr.at[0], xr.at[0], xl.at[slot]).wait()

    def norm():
        def fetch(b, slot):
            return pltpu.make_async_copy(x_ref.at[pl.ds(pl.multiple_of(b * NORM_ROWS, 8), NORM_ROWS), :], xb.at[slot], rl.at[slot])

        blocks = own // NORM_ROWS
        fetch(0, 0).start()

        def body(b, _):
            slot = lax.rem(b, 2)

            @pl.when(b + 1 < blocks)
            def _():
                fetch(b + 1, 1 - slot).start()

            fetch(b, slot).wait()
            wide = xb[slot].astype(F32)
            scale = lax.rsqrt(jnp.mean(wide * wide, -1, keepdims=True) + 1e-6)
            a_s[pl.ds(pl.multiple_of(b * NORM_ROWS, 8), NORM_ROWS), :] = (wide * scale * gain_ref[...].astype(F32)).astype(BF16)

        lax.fori_loop(0, blocks, body, None)

    def project(slot):
        def tile(t, _):
            cols = pl.ds(pl.multiple_of(t * TILE, TILE), TILE)
            t_s[:, cols] = jnp.dot(a_s[...], w_s[:, cols], preferred_element_type=F32).astype(BF16)

        lax.fori_loop(0, ccols // TILE, tile, None)

        def turned(t):
            wide = t.astype(F32)
            return (wide * cos_ref[...] + pltpu.roll(wide, HEAD // 2, 1) * sin_ref[...]).astype(BF16)

        kst[slot] = turned(t_s[:, qcols : qcols + HEAD])
        vst[slot] = t_s[:, qcols + HEAD :].astype(F32).T.astype(BF16)
        for h in range(share):
            q_s[slot, h] = turned(t_s[:, h * HEAD : (h + 1) * HEAD])

    def keys_move(g, shard, src, to, s, r):
        pltpu.make_async_remote_copy(src_ref=src, dst_ref=kall_ref.at[g, shard], send_sem=ksend.at[g, s], recv_sem=krecv.at[g, r],
                                     device_id=to, device_id_type=MESH).start()

    def values_move(g, shard, src, to, s, r):
        pltpu.make_async_remote_copy(src_ref=src, dst_ref=vall_ref.at[g, shard], send_sem=ksend.at[g, s], recv_sem=krecv.at[g, r],
                                     device_id=to, device_id_type=MESH).start()

    def kv_took(sem, arrays=2):
        view = kall_ref.at[0, pl.ds(0, arrays)]
        pltpu.make_async_copy(view, view, sem).wait()

    def f1(g, slot):
        @pl.when(me < n - 1)
        def _():
            keys_move(g, me, kst.at[slot], RIGHT, 0, 0)
            values_move(g, me, vst.at[slot], RIGHT, 0, 0)

        @pl.when(me == 0)
        def _():
            keys_move(g, me, kst.at[slot], LEFT, 1, 1)
            values_move(g, me, vst.at[slot], LEFT, 1, 1)

        @pl.when(me == 1)
        def _():
            values_move(g, me, vst.at[slot], LEFT, 1, 0)

    def f2(g):
        @pl.when(me == 0)
        def _():
            kv_took(krecv.at[g, 0], 1)
            values_move(g, right, vall_ref.at[g, right], LEFT, 2, 3)

        @pl.when(me >= 1)
        def _():
            kv_took(krecv.at[g, 0])

        @pl.when(me == n - 2)
        def _():
            keys_move(g, left, kall_ref.at[g, left], RIGHT, 1, 2)

        @pl.when(me == n - 1)
        def _():
            kv_took(krecv.at[g, 1])
            keys_move(g, right, kall_ref.at[g, right], LEFT, 1, 2)
            values_move(g, right, vall_ref.at[g, right], LEFT, 1, 2)

    def f3(g):
        @pl.when(me == n - 2)
        def _():
            kv_took(krecv.at[g, 2])

        @pl.when(me == n - 1)
        def _():
            kv_took(krecv.at[g, 2], 1)
            kv_took(krecv.at[g, 3], 1)

    def kv_sent(g):
        @pl.when(me < n - 1)
        def _():
            kv_took(ksend.at[g, 0])

        @pl.when((me == 0) | (me == n - 1))
        def _():
            kv_took(ksend.at[g, 1])

        @pl.when((me == 1) | (me == n - 2))
        def _():
            kv_took(ksend.at[g, 1], 1)

        @pl.when(me == 0)
        def _():
            kv_took(ksend.at[g, 2], 1)

    def kv_copy(j, k_src, v_src):
        here = pl.ds(pl.multiple_of(j * own, own), own)
        pltpu.make_async_copy(k_src, k_s.at[here, :], kl.at[j]).start()
        pltpu.make_async_copy(v_src, v_s.at[pl.ds(0, HEAD), here], kl.at[j]).start()

    def kv_early(g, slot):
        kv_copy(me, kst.at[slot], vst.at[slot])

        @pl.when(me >= 1)
        def _():
            kv_copy(left, kall_ref.at[g, left], vall_ref.at[g, left])

        @pl.when(me == n - 1)
        def _():
            kv_copy(right, kall_ref.at[g, right], vall_ref.at[g, right])

    def kv_late(g):
        @pl.when(me >= n - 2)
        def _():
            kv_copy(across, kall_ref.at[g, across], vall_ref.at[g, across])

    def kv_wait():
        view = k_s.at[pl.ds(0, 2 * own), :]
        for j in range(n):
            @pl.when(j <= me)
            def _():
                pltpu.make_async_copy(view, view, kl.at[j]).wait()

    per = own // STRIP
    scale = HEAD**-0.5
    e = scale * LOG2E

    def block(slot, j, strips, masked):
        here = pl.ds(pl.multiple_of(j * STRIP, STRIP), STRIP)
        keys, values = k_s[here, :], v_s[:, here]
        scores = [_dot(keys, q_s[slot, s % share, (s // share) * STRIP : (s // share + 1) * STRIP, :], 1, 1) for s in strips]
        weights, keeps = [], []
        if masked:
            ok = lax.broadcasted_iota(jnp.int32, (STRIP, STRIP), 0) <= lax.broadcasted_iota(jnp.int32, (STRIP, STRIP), 1)
        for s, score in zip(strips, scores):
            if s in masked:
                score = jnp.where(ok, score, HIDDEN)
            old = top_s[s : s + 1, :]
            top = jnp.maximum(old, score.max(axis=0, keepdims=True))
            top_s[s : s + 1, :] = top
            weights.append(jnp.exp2((score - top) * e).astype(BF16))
            keeps.append(jnp.exp2((old - top) * e))
        for s, p, keep in zip(strips, weights, keeps):
            at = slice(s * STRIP, (s + 1) * STRIP)
            mix_s[:, at] = mix_s[:, at] * keep + _dot(values, p, 1, 0)

    strips = list(range(per * share))

    def attend(slot):
        top_s[...] = jnp.full(top_s.shape, NEG, F32)
        mix_s[...] = jnp.zeros(mix_s.shape, F32)
        lax.fori_loop(0, per * me, lambda j, _: block(slot, j, strips, ()), None)

    def attend_end(g, slot):
        for d in range(per):
            block(slot, per * me + d, strips[d * share :], strips[d * share : (d + 1) * share])
        for s in strips:
            at = slice(s * STRIP, (s + 1) * STRIP)
            out = (mix_s[:HEAD, at] * (1 / mix_s[HEAD : HEAD + 1, at])).T
            seen_s[(s // share) * STRIP : (s // share + 1) * STRIP,
                   pl.ds(pl.multiple_of(g * qcols + (s % share) * HEAD, HEAD), HEAD)] = out.astype(BF16)

    event("e0", 0)
    v_s[HEAD:, :] = jnp.ones((8, n * own), BF16)
    norm()
    forward(0)
    event("e2", 0)
    forward(1)
    event("e3", 0)
    event("e2", 1)
    event("e4", 0)
    load_q(0)
    forward(2)
    event("e2", 2)

    begin = groups - BACK

    def group(it, _):
        slot = lax.rem(it, 2)
        first_o = 2 * (it - begin) - 1

        @pl.when(it >= 1)
        def _():
            f2(it - 1)
            kv_early(it - 1, 1 - slot)

        @pl.when(it < groups)
        def _():
            @pl.when(it >= 2)
            def _():
                kv_sent(it - 2)

            load_q_wait()
            project(slot)
            f1(it, slot)
            event("e3", it + 1, True)

        @pl.when(it == groups)
        def _():
            load_o(0)
            load_o(1)

        forward(it + 3)

        @pl.when(it >= begin)
        def _():
            event_o("e3", it - begin - 2)
            forward_o(first_o)

        @pl.when(it >= 1)
        def _():
            f3(it - 1)
            kv_late(it - 1)
            kv_wait()
            attend(1 - slot)

        @pl.when(it + 1 < groups)
        def _():
            event("e4", it + 1, True)
            load_q(it + 1)

        @pl.when(it >= begin)
        def _():
            event_o("e4", it - begin - 2)
            event_o("e2", first_o)
            forward_o(first_o + 1)

        @pl.when(it >= 1)
        def _():
            attend_end(it - 1, 1 - slot)

        event("e2", it + 3)

        @pl.when(it >= begin)
        def _():
            event_o("e2", first_o + 1)

    lax.fori_loop(0, groups + 1, group, None)
    done = 2 * (groups - begin) + 1
    here = groups - begin - 1

    def put(s):
        half = lax.rem(s, 2)
        return pltpu.make_async_copy(yb.at[half], y_ref.at[:, pl.ds(pl.multiple_of(s * TILE, TILE), TILE)], yl.at[half])

    pieces = width // TILE

    def last(s, _):
        c, half, slot = lax.div(s, 2), lax.rem(s, 2), lax.rem(s, 3)

        @pl.when((half == 0) & (c < no - done))
        def _():
            forward_o(c + done)

        load_o_wait(slot)

        @pl.when(s >= 2)
        def _():
            put(s - 2).wait()

        y = jnp.dot(seen_s[...], w_s[: n * rows_o, pl.ds(pl.multiple_of(slot * TILE, TILE), TILE)], preferred_element_type=F32)
        yb[half] = (xr[slot].astype(F32) + y).astype(BF16)
        put(s).start()

        @pl.when(half == 0)
        def _():
            @pl.when(c < no - done)
            def _():
                event_o("e2", c + done)

            @pl.when(c + 1 >= here)
            def _():
                event_o("e3", c + 1)
                event_o("e4", c + 1)

        @pl.when(s + 2 < pieces)
        def _():
            load_o(s + 2)

    lax.fori_loop(0, pieces, last, None)
    put(pieces - 2).wait()
    put(pieces - 1).wait()
    kv_sent(groups - 2)
    kv_sent(groups - 1)
    for c in range(EARLY):
        kf.sent(c)
    lax.fori_loop(EARLY, nq, lambda c, _: kq.sent(c), None)
    lax.fori_loop(0, no, lambda c, _: ko.sent(c), None)


def solution(mesh):
    n = mesh.shape["sp"]

    def step(x, gain, wq, wk, wv, wo):
        own, width = x.shape
        groups, share = wk.shape[1] // HEAD, wq.shape[1] // wk.shape[1]
        heads = groups * share
        nq, no = groups, width // WO_COLS
        ccols = (share + 2) * HEAD
        rows_q, rows_o = wq.shape[0], wo.shape[0]
        place = lax.axis_index("sp") * own + jnp.arange(own)
        angle = place.astype(F32)[:, None] * THETA ** (-jnp.arange(HEAD // 2, dtype=F32) / (HEAD // 2))
        cos, sin = jnp.cos(angle), jnp.sin(angle)
        cos, sin = jnp.concatenate([cos, cos], -1), jnp.concatenate([-sin, sin], -1)
        hbm, vmem = pl.BlockSpec(memory_space=pl.ANY), pl.BlockSpec(memory_space=pltpu.VMEM)
        dims = (n, groups, share, nq, no)
        dma = pltpu.SemaphoreType.DMA
        got = pl.pallas_call(
            functools.partial(kernel, dims),
            in_specs=[hbm, vmem, vmem, vmem, hbm, hbm, hbm, hbm],
            out_specs=[hbm] * 5,
            out_shape=[jax.ShapeDtypeStruct(s, BF16) for s in (
                (own, width), (nq, n, rows_q, ccols), (no, n, rows_o, WO_COLS), (groups, n, own, HEAD), (groups, n, HEAD, own))],
            scratch_shapes=[
                pltpu.VMEM((own, width), BF16),
                pltpu.VMEM((width, ccols), BF16),
                pltpu.VMEM((own, ccols), BF16),
                pltpu.VMEM((2, share, own, HEAD), BF16),
                pltpu.VMEM((2, own, HEAD), BF16),
                pltpu.VMEM((2, HEAD, own), BF16),
                pltpu.VMEM((n * own, HEAD), BF16),
                pltpu.VMEM((HEAD + 8, n * own), BF16),
                pltpu.VMEM((own, heads * HEAD), BF16),
                pltpu.VMEM((own * share // STRIP, STRIP), F32),
                pltpu.VMEM((HEAD + 8, own * share), F32),
                pltpu.VMEM((2, NORM_ROWS, width), BF16),
                pltpu.VMEM((3, own, TILE), BF16),
                pltpu.VMEM((2, own, TILE), BF16),
                dma((nq + no, 9)), dma((nq + no, 9)), dma((groups, 3)), dma((groups, 4)),
                dma((1,)), dma((3,)), dma((n,)), dma((3,)), dma((2,)), dma((2,)),
            ],
            compiler_params=pltpu.CompilerParams(collective_id=0, has_side_effects=True, vmem_limit_bytes=VMEM),
            cost_estimate=pl.CostEstimate(flops=2 * own * width * (wq.shape[1] * 2 + wk.shape[1] * 2) + 4 * own * own * n * heads * HEAD,
                                          transcendentals=own * own * n * heads, bytes_accessed=2**28),
        )(x, gain[None], cos, sin, wq, wk, wv, wo)
        return got[0]

    tokens, whole = P(("dp", "sp"), None), P("sp", None)
    return jax.shard_map(step, mesh=mesh, in_specs=(tokens, P(None), whole, whole, whole, whole), out_specs=tokens, check_vma=False)
```
